32 devices in a mesh: grp: 4 (over z), row: 4 (over y, core), col: 2 (over x).
Axes of the slice: x: 2, y: 2, z: 4, core: 2. Of those that a mesh axis runs over, the one named last changes fastest.
Arguments:
- tokens: bfloat16 [2048, 4608], P(('grp', 'row', 'col')), parts along dimension 0, may hold values from -6 to 6
- ln_gain: float32 [4608], replicated, may hold values from 0.1 to 1.9
- w_in: bfloat16 [4608, 12288], P('row', 'col'), may hold values from -0.09375 to 0.09375
- b_in: float32 [12288], P('col'), may hold values from -3 to 3
- w_out: bfloat16 [12288, 4608], P('col', 'row'), may hold values from -0.0546875 to 0.0546875
- b_out: float32 [4608], P('row'), may hold values from -3 to 3
Outputs:
- result: bfloat16 [2048, 4608], P(('grp', 'row', 'col')), parts along dimension 0
The draws below stay inside these ranges and needn't reach their ends.
There are 4 independent parts, one for each index of `grp`. The reference program is written for one: setup_inputs(seed, part) draws one part's arguments, and reference() takes and returns one part's arrays. A program takes and returns all parts, laid end to end along the dimension named above; an argument that names none is the same for every part. Nothing has to cross between parts.
All inputs are finite; a program needn't handle non-finite values.
Results may differ from the reference program's by a relative error of at most 0.0095.
Values may be sent and summed in bfloat16 or wider, within the bound.
No kernel may reach another device: no remote copies, remote signals or barrier semaphores. Data moves between devices by JAX's collectives and lax.ppermute only.
A program may use at most 128 MiB of HBM per device.

```python
import jax
import jax.numpy as jnp
from jax import lax

D = 4608
FF = 12288
TOKENS = 512


def block_scale(own_key, dims, pieces, low, top_value):
    def one(position, blocks):
        heights = jax.random.uniform(jax.random.fold_in(jax.random.fold_in(own_key, 6), position), (blocks,), jnp.float32, low / len(pieces), top_value / len(pieces))
        return jnp.repeat(jnp.exp(heights), dims[position] // blocks).reshape((-1,) + (1,) * (len(dims) - position - 1))

    loudness = one(*pieces[0])
    for cut in pieces[1:]:
        loudness = loudness * one(*cut)
    return loudness


def normal_values(rng, shape, width, limit, shards=(), held_as=jnp.bfloat16):
    drawn = width * jax.random.normal(rng, shape, jnp.float32)
    if shards:
        drawn = drawn * block_scale(rng, shape, shards, -0.22, 0.18)
    return jnp.clip(drawn, -limit, limit).astype(held_as)


def setup_inputs(seed: int = 0, part: int = 0) -> dict:
    key_list = jax.random.split(jax.random.key(seed), 7)
    own_keys = jax.random.split(jax.random.fold_in(key_list[6], part), 7)
    tokens = normal_values(own_keys[0], (TOKENS, D), 1.0, 6.0, ((0, 8),))
    ln_gain = jnp.clip(1.0 + 0.18 * jax.random.normal(key_list[1], (D,), jnp.float32), 0.1, 1.9)
    w_in = normal_values(key_list[2], (D, FF), D ** -0.5, 0.09375, ((0, 4), (1, 2)))
    b_in = normal_values(key_list[3], (FF,), 0.5, 3.0, ((0, 2),), jnp.float32)
    w_out = normal_values(key_list[4], (FF, D), FF ** -0.5, 0.0546875, ((0, 2), (1, 4)))
    b_out = normal_values(key_list[5], (D,), 0.5, 3.0, ((0, 4),), jnp.float32)
    return {"tokens": tokens, "ln_gain": ln_gain, "w_in": w_in, "b_in": b_in, "w_out": w_out, "b_out": b_out}


def reference(tokens, ln_gain, w_in, b_in, w_out, b_out):
    values = tokens.astype(jnp.float32)
    row_mean = lax.optimization_barrier(jnp.mean(values, axis=1, keepdims=True))
    centered = values - row_mean
    row_var = lax.optimization_barrier(jnp.mean(centered * centered, axis=1, keepdims=True))
    normed = (centered * jax.lax.rsqrt(row_var + 1e-06) * ln_gain).astype(jnp.bfloat16)
    preact = jnp.dot(normed, w_in, preferred_element_type=jnp.float32) + b_in
    hidden = jax.nn.gelu(preact, approximate=False).astype(jnp.bfloat16)
    branch_out = (jnp.dot(hidden, w_out, preferred_element_type=jnp.float32) + b_out).astype(jnp.bfloat16)
    return (values + branch_out.astype(jnp.float32)).astype(jnp.bfloat16)
```

```python
import jax
import jax.numpy as jnp
from jax import lax
from jax.sharding import PartitionSpec as P


def swap(value, axis, size, mask):
    return lax.ppermute(value, axis, [(i, i ^ mask) for i in range(size)])


def pick(blocks, index, slot):
    bits = len(blocks).bit_length() - 1

    def choose(bit, done):
        if bit == bits:
            return blocks[slot ^ done]
        on = (index >> bit) & 1
        return jnp.where(on == 1, choose(bit + 1, done | (1 << bit)), choose(bit + 1, done))

    return choose(0, 0)


def solution(mesh):
    rows, cols = mesh.shape["row"], mesh.shape["col"]
    row_bits = rows.bit_length() - 1
    order = [0]
    for bit in reversed(range(row_bits)):
        order = order + [p | (1 << bit) for p in order]

    def local(tokens, ln_gain, w_in, b_in, w_out, b_out):
        own = tokens.shape[0]
        width = w_in.shape[0]
        row = lax.axis_index("row")
        values = tokens.astype(jnp.float32)
        row_mean = jnp.mean(values, axis=1, keepdims=True)
        centered = values - row_mean
        row_var = jnp.mean(centered * centered, axis=1, keepdims=True)
        normed = (centered * lax.rsqrt(row_var + 1e-06) * ln_gain).astype(jnp.bfloat16)

        def slab(p):
            return lax.dynamic_slice_in_dim(normed, (row ^ p) * width, width, axis=1)

        panel = jnp.concatenate([slab(0) if p == 0 else swap(slab(p), "row", rows, p) for p in order])
        panels = {q: panel if q == 0 else swap(panel, "col", cols, q) for q in range(cols)}

        cut = w_in.shape[1] // 2
        halves = [slice(0, cut), slice(cut, 2 * cut)]
        steps = [(0, 0)] + [(q, f) for q in range(1, cols) for f in range(2)] + [(0, 1)]
        partial = {}
        for q, f in steps:
            value = jnp.dot(panels[q], w_in[:, halves[f]], preferred_element_type=jnp.float32).astype(jnp.bfloat16)
            for bit in range(row_bits):
                half = value.shape[0] // 2
                got = swap(value[half:], "row", rows, 1 << bit)
                value = value[:half].astype(jnp.float32) + got.astype(jnp.float32)
                if bit < row_bits - 1:
                    value = value.astype(jnp.bfloat16)
            hidden = jax.nn.gelu(value + b_in[halves[f]], approximate=False).astype(jnp.bfloat16)
            for bit in reversed(range(row_bits)):
                hidden = jnp.concatenate([hidden, swap(hidden, "row", rows, 1 << bit)])
            part = jnp.dot(hidden, w_out[halves[f]], preferred_element_type=jnp.float32)
            partial[q] = part if q not in partial else partial[q] + part

        summed = partial[0]
        for q in range(1, cols):
            summed = summed + swap(partial[q].astype(jnp.bfloat16), "col", cols, q).astype(jnp.float32)
        branch_out = (summed + b_out).astype(jnp.bfloat16)
        blocks = {}
        for place, p in enumerate(order):
            block = branch_out[place * own : (place + 1) * own]
            blocks[p] = block if p == 0 else swap(block, "row", rows, p)
        regrouped = jnp.concatenate([pick(blocks, row, s) for s in range(rows)], axis=1)
        return (values + regrouped.astype(jnp.float32)).astype(jnp.bfloat16)

    in_specs = (
        P(("grp", "row", "col"), None),
        P(),
        P("row", "col"),
        P("col"),
        P("col", "row"),
        P("row"),
    )
    out_specs = P(("grp", "row", "col"), None)
    return jax.shard_map(local, mesh=mesh, in_specs=in_specs, out_specs=out_specs, check_vma=False)
```

```python
import jax
import jax.numpy as jnp
from jax import lax
from jax.sharding import PartitionSpec as P


def swap(value, axis, size, mask):
    return lax.ppermute(value, axis, [(i, i ^ mask) for i in range(size)])


def pick(blocks, index, slot):
    bits = len(blocks).bit_length() - 1

    def choose(bit, done):
        if bit == bits:
            return blocks[slot ^ done]
        on = (index >> bit) & 1
        return jnp.where(on == 1, choose(bit + 1, done | (1 << bit)), choose(bit + 1, done))

    return choose(0, 0)


def solution(mesh):
    rows, cols = mesh.shape["row"], mesh.shape["col"]
    low_bits = rows.bit_length() - 2
    top = rows // 2
    near = [0]
    for bit in reversed(range(low_bits)):
        near = near + [p | (1 << bit) for p in near]
    far = [p | top for p in near]

    def low_reduce(value):
        for bit in range(low_bits):
            half = value.shape[0] // 2
            got = swap(value[half:], "row", rows, 1 << bit)
            value = (value[:half].astype(jnp.float32) + got.astype(jnp.float32)).astype(jnp.bfloat16)
        return value

    def low_gather(value):
        for bit in reversed(range(low_bits)):
            value = jnp.concatenate([value, swap(value, "row", rows, 1 << bit)])
        return value

    def local(tokens, ln_gain, w_in, b_in, w_out, b_out):
        width = w_in.shape[0]
        row = lax.axis_index("row")
        values = tokens.astype(jnp.float32)
        row_mean = jnp.mean(values, axis=1, keepdims=True)
        centered = values - row_mean
        row_var = jnp.mean(centered * centered, axis=1, keepdims=True)
        normed = (centered * lax.rsqrt(row_var + 1e-06) * ln_gain).astype(jnp.bfloat16)

        def slab(p):
            return lax.dynamic_slice_in_dim(normed, (row ^ p) * width, width, axis=1)

        near_own = jnp.concatenate([slab(p) if p == 0 else swap(slab(p), "row", rows, p) for p in near])
        far_own = jnp.concatenate([swap(slab(p), "row", rows, p) for p in far])
        near_in = [near_own if q == 0 else swap(near_own, "col", cols, q) for q in range(cols)]
        far_in = [far_own if q == 0 else swap(far_own, "col", cols, q) for q in range(cols)]

        full = w_in.shape[1]
        whole = [slice(0, full)]
        halves = [slice(0, full // 2), slice(full // 2, full)]

        def up(panel, cut):
            return jnp.dot(panel, w_in[:, cut], preferred_element_type=jnp.float32).astype(jnp.bfloat16)

        def down(hidden, cut):
            return jnp.dot(hidden, w_out[cut], preferred_element_type=jnp.float32)

        near_out, far_out = [None] * cols, [None] * cols
        hidden = [None] * cols
        for q in range(cols):
            cuts = halves if q == 0 else whole
            hidden[q] = []
            for cut in cuts:
                away = swap(low_reduce(up(near_in[q], cut)), "row", rows, top)
                kept = low_reduce(up(far_in[q], cut))
                preact = kept.astype(jnp.float32) + away.astype(jnp.float32) + b_in[cut]
                hidden[q].append(jax.nn.gelu(preact, approximate=False).astype(jnp.bfloat16))
            far_out[q] = sum(down(low_gather(h), cut) for h, cut in zip(hidden[q], cuts))
        for q in reversed(range(cols)):
            cuts = halves if q == 0 else whole
            near_out[q] = sum(down(low_gather(swap(h, "row", rows, top)), cut) for h, cut in zip(hidden[q], cuts))

        def finish(parts):
            total = parts[0]
            for q in range(1, cols):
                total = total + swap(parts[q].astype(jnp.bfloat16), "col", cols, q).astype(jnp.float32)
            return (total + b_out).astype(jnp.bfloat16)

        blocks = {}
        own = tokens.shape[0]
        for names, branch in ((far, finish(far_out)), (near, finish(near_out))):
            for place, p in enumerate(names):
                block = branch[place * own : (place + 1) * own]
                blocks[p] = block if p == 0 else swap(block, "row", rows, p)
        regrouped = jnp.concatenate([pick(blocks, row, s) for s in range(rows)], axis=1)
        return (values + regrouped.astype(jnp.float32)).astype(jnp.bfloat16)

    in_specs = (
        P(("grp", "row", "col"), None),
        P(),
        P("row", "col"),
        P("col"),
        P("col", "row"),
        P("row"),
    )
    out_specs = P(("grp", "row", "col"), None)

    return jax.shard_map(local, mesh=mesh, in_specs=in_specs, out_specs=out_specs, check_vma=False)
```

```python
import jax
import jax.numpy as jnp
from jax import lax
from jax.sharding import PartitionSpec as P


def swap(value, axis, size, mask):
    return lax.ppermute(value, axis, [(i, i ^ mask) for i in range(size)])


def after(value, other):
    return value if other is None else lax.optimization_barrier((value, other))[0]


def pick(blocks, index, slot):
    bits = len(blocks).bit_length() - 1

    def choose(bit, done):
        if bit == bits:
            return blocks[slot ^ done]
        on = (index >> bit) & 1
        return jnp.where(on == 1, choose(bit + 1, done | (1 << bit)), choose(bit + 1, done))

    return choose(0, 0)


def solution(mesh):
    rows, cols = mesh.shape["row"], mesh.shape["col"]
    low_bits = rows.bit_length() - 2
    top = rows // 2
    near = [0]
    for bit in reversed(range(low_bits)):
        near = near + [p | (1 << bit) for p in near]
    far = [p | top for p in near]

    def low_reduce(value):
        for bit in range(low_bits):
            half = value.shape[0] // 2
            got = swap(value[half:], "row", rows, 1 << bit)
            value = (value[:half].astype(jnp.float32) + got.astype(jnp.float32)).astype(jnp.bfloat16)
        return value

    def low_gather(value):
        for bit in reversed(range(low_bits)):
            value = jnp.concatenate([value, swap(value, "row", rows, 1 << bit)])
        return value

    def local(tokens, ln_gain, w_in, b_in, w_out, b_out):
        width = w_in.shape[0]
        row = lax.axis_index("row")
        values = tokens.astype(jnp.float32)
        row_mean = jnp.mean(values, axis=1, keepdims=True)
        centered = values - row_mean
        row_var = jnp.mean(centered * centered, axis=1, keepdims=True)
        normed = (centered * lax.rsqrt(row_var + 1e-06) * ln_gain).astype(jnp.bfloat16)

        def slab(p):
            return lax.dynamic_slice_in_dim(normed, (row ^ p) * width, width, axis=1)

        near_own = jnp.concatenate([slab(p) if p == 0 else swap(slab(p), "row", rows, p) for p in near])
        far_own = jnp.concatenate([swap(slab(p), "row", rows, p) for p in far])
        near_in = [near_own if q == 0 else swap(near_own, "col", cols, q) for q in range(cols)]
        far_in = [far_own if q == 0 else swap(far_own, "col", cols, q) for q in range(cols)]

        full = w_in.shape[1]
        whole = [slice(0, full)]
        halves = [slice(0, full // 2), slice(full // 2, full)]

        def up(panel, cut):
            return jnp.dot(panel, w_in[:, cut], preferred_element_type=jnp.float32).astype(jnp.bfloat16)

        def down(hidden, cut):
            return jnp.dot(hidden, w_out[cut], preferred_element_type=jnp.float32)

        near_out, far_out = [None] * cols, [None] * cols
        hidden = [None] * cols
        for q in range(cols):
            cuts = halves if q == 0 else whole
            hidden[q] = []
            sent = None
            for cut in cuts:
                sent = low_reduce(up(after(near_in[q], sent), cut))
                away = swap(sent, "row", rows, top)
                kept = low_reduce(up(far_in[q], cut))
                preact = kept.astype(jnp.float32) + away.astype(jnp.float32) + b_in[cut]
                hidden[q].append(jax.nn.gelu(preact, approximate=False).astype(jnp.bfloat16))
            far_out[q] = sum(down(low_gather(h), cut) for h, cut in zip(hidden[q], cuts))
        for q in reversed(range(cols)):
            cuts = halves if q == 0 else whole
            total = None
            for h, cut in zip(hidden[q], cuts):
                back = after(swap(h, "row", rows, top), total)
                part = down(low_gather(back), cut)
                total = part if total is None else total + part
            near_out[q] = total

        def finish(parts):
            total = parts[0]
            for q in range(1, cols):
                total = total + swap(parts[q].astype(jnp.bfloat16), "col", cols, q).astype(jnp.float32)
            return (total + b_out).astype(jnp.bfloat16)

        blocks = {}
        own = tokens.shape[0]
        for names, branch in ((far, finish(far_out)), (near, finish(near_out))):
            for place, p in enumerate(names):
                block = branch[place * own : (place + 1) * own]
                blocks[p] = block if p == 0 else swap(block, "row", rows, p)
        regrouped = jnp.concatenate([pick(blocks, row, s) for s in range(rows)], axis=1)
        return (values + regrouped.astype(jnp.float32)).astype(jnp.bfloat16)

    in_specs = (
        P(("grp", "row", "col"), None),
        P(),
        P("row", "col"),
        P("col"),
        P("col", "row"),
        P("row"),
    )
    out_specs = P(("grp", "row", "col"), None)

    return jax.shard_map(local, mesh=mesh, in_specs=in_specs, out_specs=out_specs, check_vma=False)
```
